32 devices in a mesh: grp: 4 (over y, x), tp: 8 (over z, core).
Axes of the slice: x: 2, y: 2, z: 4, core: 2. Of those that a mesh axis runs over, the one named last changes fastest.
Arguments:
- key_cache: bfloat16 [4, 8, 768, 512], P('grp', 'tp'), may hold values from -6 to 6
- value_cache: bfloat16 [4, 8, 768, 512], P('grp', 'tp'), may hold values from -12 to 12
- lengths: int32 [4, 8], P('grp', 'tp'), may hold values from 256 to 768, as said below
- queries: bfloat16 [4, 1, 8, 8192], P('grp', None, 'tp'), may hold values from -12 to 12
- new_keys: bfloat16 [4, 1, 8, 512], P('grp', None, 'tp'), may hold values from -18 to 18
- new_values: bfloat16 [4, 1, 8, 512], P('grp', None, 'tp'), may hold values from -12 to 12
- residual: bfloat16 [4, 1, 8, 8192], P('grp', None, 'tp'), may hold values from -4 to 4
- norm_gain: float32 [8192], replicated, may hold values from 0.25 to 1.75
- gate_weight: bfloat16 [4, 13312, 8192], P('grp', 'tp'), may hold values from -0.0625 to 0.0625
- up_weight: bfloat16 [4, 13312, 8192], P('grp', 'tp'), may hold values from -0.0625 to 0.0625
- down_weight: bfloat16 [4, 13312, 8192], P('grp', 'tp'), may hold values from -0.0390625 to 0.0390625
Outputs:
- mixed: bfloat16 [4, 1, 8, 8192], P('grp', None, 'tp')
The draws below stay inside these ranges and needn't reach their ends.
Inputs may be any that keep to these rules, and one draw needn't show every extreme that they name: `lengths`: some row has exactly 768 valid positions.
All inputs are finite; a program needn't handle non-finite values.
Results may differ from the reference program's by a relative error of at most 0.005.
Values may be sent and summed in bfloat16 or wider, within the bound.
A program may use at most 128 MiB of HBM per device.

```python
import jax
import jax.numpy as jnp
from jax import lax

D = 8192
HEADS = 64
HD = 128
KVH = 4
FF = 26624
CAP = 768
STEPS = 1
AGROUPS = 2
GROUP_ROWS = 8
N_GRP = 4


def draw_key_cache(key, part):
    shape = (N_GRP, GROUP_ROWS, CAP, KVH * HD)
    base = jax.random.truncated_normal(jax.random.fold_in(key, 11), -6.0, 6.0, shape)
    return base.astype(jnp.bfloat16)


def draw_queries(key, part):
    shape = (N_GRP, STEPS, GROUP_ROWS, D)
    base = 2.5 * jax.random.truncated_normal(jax.random.fold_in(key, 12), -4.8, 4.8, shape)
    return base.astype(jnp.bfloat16)


def draw_lengths(key, part):
    reach = CAP // 3
    spread = jax.random.randint(jax.random.fold_in(key, 21), (N_GRP, GROUP_ROWS), 0, CAP - reach + 1)
    group = jnp.arange(N_GRP) % (N_GRP // 2)
    length = reach + spread * (group[:, None] + 1) // (N_GRP // 2)
    peak_row = jax.random.randint(jax.random.fold_in(key, 22), (), 0, GROUP_ROWS)
    mark = (jnp.arange(N_GRP)[:, None] == N_GRP // 2 - 1) & (jnp.arange(GROUP_ROWS)[None, :] == peak_row)
    return jnp.where(mark, CAP, length).astype(jnp.int32)


def draw_residual(key, part):
    shape = (N_GRP, STEPS, GROUP_ROWS, D)
    base = jax.random.truncated_normal(jax.random.fold_in(key, 31), -6.0, 6.0, shape)
    return (0.5 * base).astype(jnp.bfloat16)


def levels(own_key, extent, cuts, low, high):
    factor_of = 1.0
    for dim, shards_of in cuts:
        draws = jax.random.uniform(jax.random.fold_in(jax.random.fold_in(own_key, 6), dim), (shards_of,), jnp.float32, low / len(cuts), high / len(cuts))
        factor_of = factor_of * jnp.repeat(jnp.exp(draws), extent[dim] // shards_of).reshape((-1,) + (1,) * (len(extent) - 1 - dim))
    return factor_of


def scatter_about(key, dims, scale, limit, shards=(), held_as=jnp.bfloat16):
    loudness = levels(key, dims, shards, -0.22, 0.18) if shards else 1.0
    values = jax.random.normal(key, dims, jnp.float32) * scale * loudness
    return jnp.minimum(jnp.maximum(values, -limit), limit).astype(held_as)


def setup_inputs(seed: int = 0) -> dict:
    splits = jax.random.split(jax.random.key(seed), 12)
    return {
        "key_cache": draw_key_cache(jax.random.fold_in(splits[11], 71), 0),
        "value_cache": scatter_about(splits[1], (N_GRP, GROUP_ROWS, CAP, KVH * HD), 2.0, 12.0, ((0, 4), (1, 8))),
        "lengths": draw_lengths(jax.random.fold_in(splits[11], 71), 0),
        "queries": draw_queries(jax.random.fold_in(splits[11], 71), 0),
        "new_keys": scatter_about(splits[4], (N_GRP, STEPS, GROUP_ROWS, KVH * HD), 3.0, 18.0, ((0, 4), (2, 8))),
        "new_values": scatter_about(splits[5], (N_GRP, STEPS, GROUP_ROWS, KVH * HD), 2.0, 12.0, ((0, 4), (2, 8))),
        "residual": draw_residual(jax.random.fold_in(splits[11], 71), 0),
        "norm_gain": jnp.clip(1.0 + 0.15 * jax.random.normal(splits[7], (D,), jnp.float32), 0.25, 1.75),
        "gate_weight": scatter_about(splits[8], (N_GRP, FF // AGROUPS, D), D ** -0.5, 0.0625, ((0, 4), (1, 8))),
        "up_weight": scatter_about(splits[9], (N_GRP, FF // AGROUPS, D), D ** -0.5, 0.0625, ((0, 4), (1, 8))),
        "down_weight": scatter_about(splits[10], (N_GRP, FF // AGROUPS, D), FF ** -0.5, 0.0390625, ((0, 4), (1, 8))),
    }


masked_score = -1e+30

def attend_row(row_inputs):
    cache_keys, cache_values, length, query_rows, fresh_keys, fresh_values = row_inputs
    head_share = HEADS // KVH
    score_scale = HD ** (-0.5)
    query_wide = query_rows.astype(jnp.float32).reshape(STEPS, KVH, head_share, HD)
    keys_wide = cache_keys.astype(jnp.float32).reshape(CAP, KVH, HD)
    values_wide = cache_values.astype(jnp.float32).reshape(CAP, KVH, HD)
    fresh_keys_wide = fresh_keys.astype(jnp.float32).reshape(STEPS, KVH, HD)
    fresh_values_wide = fresh_values.astype(jnp.float32).reshape(STEPS, KVH, HD)
    usable = jnp.arange(CAP) < length
    cache_scores = jnp.einsum('sjgd,pjd->sjgp', query_wide, keys_wide) * score_scale
    cache_scores = jnp.where(usable, cache_scores, masked_score)
    causal = jnp.arange(STEPS)[:, None] >= jnp.arange(STEPS)[None, :]
    causal_mask = causal[:, None, None, :]
    fresh_scores = jnp.einsum('sjgd,tjd->sjgt', query_wide, fresh_keys_wide) * score_scale
    fresh_scores = jnp.where(causal_mask, fresh_scores, masked_score)
    ceiling = jnp.maximum(lax.optimization_barrier(jnp.max(cache_scores, axis=-1)), lax.optimization_barrier(jnp.max(fresh_scores, axis=-1)))
    cache_exp = jnp.where(usable, jnp.exp(cache_scores - ceiling[..., None]), 0.0)
    fresh_exp = jnp.where(causal_mask, jnp.exp(fresh_scores - ceiling[..., None]), 0.0)
    denominator = lax.optimization_barrier(jnp.sum(cache_exp, axis=-1)) + lax.optimization_barrier(jnp.sum(fresh_exp, axis=-1))
    cache_weights = lax.optimization_barrier(cache_exp.astype(jnp.bfloat16)).astype(jnp.float32)
    fresh_weights = lax.optimization_barrier(fresh_exp.astype(jnp.bfloat16)).astype(jnp.float32)
    weighted = jnp.einsum('sjgp,pjd->sjgd', cache_weights, values_wide)
    weighted = weighted + jnp.einsum('sjgt,tjd->sjgd', fresh_weights, fresh_values_wide)
    return (weighted / denominator[..., None]).reshape(STEPS, HEADS * HD)

def reference(key_cache, value_cache, lengths, queries, new_keys, new_values, residual, norm_gain, gate_weight, up_weight, down_weight):
    row_total = AGROUPS * GROUP_ROWS
    cache_keys = key_cache[:AGROUPS].reshape(row_total, CAP, KVH * HD)
    cache_values = value_cache[:AGROUPS].reshape(row_total, CAP, KVH * HD)
    row_lengths = lengths[:AGROUPS].reshape(row_total)
    query_rows = jnp.swapaxes(queries[:AGROUPS], 1, 2).reshape(row_total, STEPS, D)
    fresh_keys = jnp.swapaxes(new_keys[:AGROUPS], 1, 2).reshape(row_total, STEPS, KVH * HD)
    fresh_values = jnp.swapaxes(new_values[:AGROUPS], 1, 2).reshape(row_total, STEPS, KVH * HD)
    attended = lax.map(attend_row, (cache_keys, cache_values, row_lengths, query_rows, fresh_keys, fresh_values))
    attended = jnp.swapaxes(attended.reshape(AGROUPS, GROUP_ROWS, STEPS, D), 1, 2)
    hidden = residual[:AGROUPS].astype(jnp.float32) + attended
    spread_sq = lax.optimization_barrier(jnp.mean(hidden * hidden, axis=-1, keepdims=True))
    normed = (hidden * lax.rsqrt(spread_sq + 1e-05) * norm_gain).astype(jnp.bfloat16)
    flat_rows = normed.reshape(-1, D)
    numbers = (((1,), (1,)), ((), ()))
    gate_part = lax.dot_general(flat_rows, gate_weight[AGROUPS:].reshape(FF, D), numbers, preferred_element_type=jnp.float32)
    up_part = lax.dot_general(flat_rows, up_weight[AGROUPS:].reshape(FF, D), numbers, preferred_element_type=jnp.float32)
    product = (jax.nn.silu(gate_part) * up_part).astype(jnp.bfloat16)
    feed = jnp.dot(product, down_weight[AGROUPS:].reshape(FF, D), preferred_element_type=jnp.float32)
    mixed = (hidden + feed.reshape(hidden.shape)).astype(jnp.bfloat16)
    return jnp.concatenate([mixed, jnp.zeros_like(mixed)], axis=0)
```

```python
import functools

import jax
import jax.numpy as jnp
from jax import lax
from jax.experimental import pallas as pl
from jax.experimental.pallas import tpu as pltpu
from jax.sharding import PartitionSpec as P

HEADS = 64
HD = 128
KVH = 4
SHARE = HEADS // KVH

masked_score = -1e30
MESH_ID = pl.DeviceIdType.MESH
VMEM_BYTES = 66_000_000


def kernel(
    plan,
    lengths,
    queries,
    fresh_keys,
    fresh_values,
    residual,
    gain,
    key_hbm,
    value_hbm,
    gate_hbm,
    up_hbm,
    down_hbm,
    out,
    keys,
    values,
    hidden,
    normed,
    box,
    wide,
    rows,
    act,
    part,
    slots,
    down_slots,
    cache_sem,
    slot_sem,
    down_sem,
    send_sem,
    recv_sem,
):
    (half, members, chunk, chunks, ring, down_cols, down_chunks, down_ring, batch) = plan
    peers = half * members
    blocks = HEADS
    group = lax.axis_index("grp")
    member = lax.axis_index("tp")
    serving = group < half
    mine = lax.rem(group, half) * members + member
    other = jnp.where(serving, half, 0)
    barrier = pltpu.get_barrier_semaphore()

    def peer_id(i):
        return {"grp": other + i // members, "tp": lax.rem(i, members)}

    def slot_copies(i, s):
        start = pl.multiple_of(i * chunk, chunk)
        return (
            pltpu.make_async_copy(
                gate_hbm.at[0, pl.ds(start, chunk), :], slots.at[s, 0], slot_sem.at[s]
            ),
            pltpu.make_async_copy(
                up_hbm.at[0, pl.ds(start, chunk), :], slots.at[s, 1], slot_sem.at[s]
            ),
        )

    def down_copy(c, s):
        start = pl.multiple_of(c * down_cols, down_cols)
        return pltpu.make_async_copy(
            down_hbm.at[0, :, pl.ds(start, down_cols)], down_slots.at[s], down_sem.at[s]
        )

    key_copy = pltpu.make_async_copy(key_hbm.at[0, 0], keys, cache_sem.at[0])
    value_copy = pltpu.make_async_copy(value_hbm.at[0, 0], values, cache_sem.at[1])

    @pl.when(serving)
    def _():
        key_copy.start()
        value_copy.start()

    @pl.when(jnp.logical_not(serving))
    def _():
        for i in range(min(ring, chunks)):
            for copy in slot_copies(i, i):
                copy.start()

    @pl.loop(0, peers)
    def _(i):
        pl.semaphore_signal(barrier, inc=1, device_id=peer_id(i), device_id_type=MESH_ID)

    @pl.when(serving)
    def _():
        slot_count = keys.shape[0]
        scale = HD ** (-0.5)
        usable = lax.broadcasted_iota(jnp.int32, (SHARE, slot_count), 1) < lengths[0, 0]
        key_copy.wait()
        value_copy.wait()
        spread = jnp.zeros((1, 1), jnp.float32)
        for j in range(KVH):
            head = slice(j * SHARE, (j + 1) * SHARE)
            lanes = slice(j * HD, (j + 1) * HD)
            own = queries[head, :]
            scores = (
                lax.dot_general(
                    own, keys[:, lanes], (((1,), (1,)), ((), ())),
                    preferred_element_type=jnp.float32,
                )
                * scale
            )
            scores = jnp.where(usable, scores, masked_score)
            fresh = (
                jnp.sum(
                    own.astype(jnp.float32) * fresh_keys[j : j + 1, :].astype(jnp.float32),
                    axis=-1, keepdims=True,
                )
                * scale
            )
            ceiling = jnp.maximum(jnp.max(scores, axis=-1, keepdims=True), fresh)
            expo = jnp.where(usable, jnp.exp(scores - ceiling), 0.0)
            fresh_expo = jnp.exp(fresh - ceiling)
            denominator = jnp.sum(expo, axis=-1, keepdims=True) + fresh_expo
            total = jnp.dot(
                expo.astype(jnp.bfloat16), values[:, lanes], preferred_element_type=jnp.float32
            )
            total = total + fresh_expo.astype(jnp.bfloat16).astype(jnp.float32) * fresh_values[
                j : j + 1, :
            ].astype(jnp.float32)
            row = residual[head, :].astype(jnp.float32) + total / denominator
            hidden[head, :] = row
            squares = jnp.sum(row * row, axis=-1, keepdims=True)
            spread = spread + jnp.sum(squares, axis=0, keepdims=True)
        factor = lax.rsqrt(spread / (HEADS * HD) + 1e-05)
        normed[...] = (hidden[...] * factor * gain[...]).astype(jnp.bfloat16)
        pl.semaphore_wait(barrier, peers)

        @pl.loop(0, peers)
        def _(i):
            to = lax.rem(mine + i, peers)
            pltpu.make_async_remote_copy(
                src_ref=normed,
                dst_ref=box.at[mine],
                send_sem=send_sem,
                recv_sem=recv_sem,
                device_id=peer_id(to),
                device_id_type=MESH_ID,
            ).start()

        pltpu.make_async_copy(box, box, send_sem).wait()
        pltpu.make_async_copy(box, box, recv_sem).wait()

        for b in range(0, blocks, batch):
            band = slice(b, b + batch)
            total = hidden[band, :]
            feed = lax.fori_loop(
                0,
                peers,
                lambda f, so_far: so_far + box[f, band, :].astype(jnp.float32),
                jnp.zeros_like(total),
            )
            out[band, :] = (total + feed).astype(jnp.bfloat16)

    @pl.when(jnp.logical_not(serving))
    def _():
        out[...] = jnp.zeros_like(out)
        pl.semaphore_wait(barrier, peers)
        pltpu.make_async_copy(box, box, recv_sem).wait()
        for c in range(min(down_ring, down_chunks)):
            down_copy(c, c).start()

        @pl.loop(0, peers)
        def _(r):
            wide[pl.ds(pl.multiple_of(r * blocks, blocks), blocks), :] = box[r].astype(jnp.float32)

        for h in range(blocks):
            rows[:, h * HD : (h + 1) * HD] = wide[pl.ds(h, peers, stride=blocks), :].astype(
                jnp.bfloat16
            )

        numbers = (((1,), (1,)), ((), ()))

        def product(weights):
            mid = weights.shape[1] // 2
            return lax.dot_general(
                rows[:, :mid], weights[:, :mid], numbers, preferred_element_type=jnp.float32
            ) + lax.dot_general(
                rows[:, mid:], weights[:, mid:], numbers, preferred_element_type=jnp.float32
            )

        def hidden_units(i, s):
            pltpu.make_async_copy(slots.at[s], slots.at[s], slot_sem.at[s]).wait()
            gate = product(slots[s, 0])
            up = product(slots[s, 1])
            return (gate / (1.0 + jnp.exp(-gate)) * up).astype(jnp.bfloat16)

        if chunks == 1:
            act[...] = hidden_units(0, 0)
        else:

            @pl.loop(0, chunks)
            def _(i):
                s = lax.rem(i, ring)
                act[:, pl.ds(pl.multiple_of(i * chunk, chunk), chunk)] = hidden_units(i, s)

                @pl.when(i + ring < chunks)
                def _():
                    for copy in slot_copies(i + ring, s):
                        copy.start()

        per_chunk = down_cols // HD
        per_send = batch // per_chunk

        @pl.loop(0, down_chunks // per_send)
        def _(g):
            base = pl.multiple_of(g * batch, batch)
            for k in range(per_send):
                c = g * per_send + k
                s = lax.rem(c, down_ring)
                pltpu.make_async_copy(down_slots.at[s], down_slots.at[s], down_sem.at[s]).wait()
                feed = jnp.dot(act[...], down_slots[s], preferred_element_type=jnp.float32)

                @pl.when(c + down_ring < down_chunks)
                def _():
                    down_copy(c + down_ring, s).start()

                for h in range(per_chunk):
                    wide[pl.ds(base + k * per_chunk + h, peers, stride=blocks), :] = feed[
                        :, h * HD : (h + 1) * HD
                    ]

            @pl.loop(0, peers)
            def _(r):
                start = pl.multiple_of(r * blocks + base, batch)
                part[r, pl.ds(base, batch), :] = wide[pl.ds(start, batch), :].astype(jnp.bfloat16)

            @pl.loop(0, peers)
            def _(i):
                to = lax.rem(mine + i, peers)
                pltpu.make_async_remote_copy(
                    src_ref=part.at[to, pl.ds(base, batch), :],
                    dst_ref=box.at[mine, pl.ds(base, batch), :],
                    send_sem=send_sem,
                    recv_sem=recv_sem,
                    device_id=peer_id(to),
                    device_id_type=MESH_ID,
                ).start()

        pltpu.make_async_copy(part, part, send_sem).wait()


def local(
    key_cache,
    value_cache,
    lengths,
    queries,
    new_keys,
    new_values,
    residual,
    norm_gain,
    gate_weight,
    up_weight,
    down_weight,
):
    groups = lax.axis_size("grp")
    members = lax.axis_size("tp")
    half = groups // 2
    peers = half * members
    width = queries.shape[3]
    slot_count = key_cache.shape[2]
    units = gate_weight.shape[1]
    chunk = HD if units % HD == 0 else units
    chunks = units // chunk
    slot_bytes = 4 * chunk * width
    ring = max(1, min(chunks, 42_000_000 // slot_bytes))
    down_cols = 512
    down_chunks = width // down_cols
    down_ring = min(down_chunks, max(1, 14_000_000 // (2 * units * down_cols)))
    batch = 16
    plan = (half, members, chunk, chunks, ring, down_cols, down_chunks, down_ring, batch)
    vmem = pl.BlockSpec(memory_space=pltpu.VMEM)
    any_space = pl.BlockSpec(memory_space=pl.ANY)
    bf16 = jnp.bfloat16
    f32 = jnp.float32
    mixed = pl.pallas_call(
        functools.partial(kernel, plan),
        out_shape=jax.ShapeDtypeStruct((HEADS, HD), bf16),
        in_specs=[pl.BlockSpec(memory_space=pltpu.SMEM)] + [vmem] * 5 + [any_space] * 5,
        out_specs=vmem,
        scratch_shapes=[
            pltpu.VMEM((slot_count, KVH * HD), bf16),
            pltpu.VMEM((slot_count, KVH * HD), bf16),
            pltpu.VMEM((HEADS, HD), f32),
            pltpu.VMEM((HEADS, HD), bf16),
            pltpu.VMEM((peers, HEADS, HD), bf16),
            pltpu.VMEM((peers * HEADS, HD), f32),
            pltpu.VMEM((peers, width), bf16),
            pltpu.VMEM((peers, units), bf16),
            pltpu.VMEM((peers, HEADS, HD), bf16),
            pltpu.VMEM((ring, 2, chunk, width), bf16),
            pltpu.VMEM((down_ring, units, down_cols), bf16),
            pltpu.SemaphoreType.DMA((2,)),
            pltpu.SemaphoreType.DMA((ring,)),
            pltpu.SemaphoreType.DMA((down_ring,)),
            pltpu.SemaphoreType.DMA,
            pltpu.SemaphoreType.DMA,
        ],
        compiler_params=pltpu.CompilerParams(
            collective_id=0, has_side_effects=True, vmem_limit_bytes=VMEM_BYTES
        ),
    )(
        lengths,
        queries.reshape(HEADS, HD),
        new_keys.reshape(KVH, HD),
        new_values.reshape(KVH, HD),
        residual.reshape(HEADS, HD),
        norm_gain.reshape(HEADS, HD),
        key_cache,
        value_cache,
        gate_weight,
        up_weight,
        down_weight,
    )
    return mixed.reshape(1, 1, 1, width)


def solution(mesh):
    return jax.shard_map(
        local,
        mesh=mesh,
        in_specs=(
            P("grp", "tp", None, None),
            P("grp", "tp", None, None),
            P("grp", "tp"),
            P("grp", None, "tp", None),
            P("grp", None, "tp", None),
            P("grp", None, "tp", None),
            P("grp", None, "tp", None),
            P(),
            P("grp", "tp", None),
            P("grp", "tp", None),
            P("grp", "tp", None),
        ),
        out_specs=P("grp", None, "tp", None),
        check_vma=False,
    )
```
